32 devices in a mesh: groups: 2 (over y), tensor: 4 (over z), dp: 2 (over x), seq: 2 (over core).
Axes of the slice: x: 2, y: 2, z: 4, core: 2. Of those that a mesh axis runs over, the one named last changes fastest.
Arguments:
- attn_heads: bfloat16 [256, 8192], P(('groups', 'dp', 'seq'), 'tensor'), parts along dimension 0, may hold values from -6 to 6
- out_weight: bfloat16 [8192, 8192], P(('tensor', 'seq')), may hold values from -0.09375 to 0.09375
- residual: bfloat16 [256, 8192], P(('groups', 'dp', 'seq'), 'tensor'), parts along dimension 0, may hold values from -32 to 32
- norm_gain: bfloat16 [8192], P('tensor'), may hold values from 0.099609375 to 1.8984375
Outputs:
- stream: bfloat16 [256, 8192], P(('groups', 'dp', 'seq'), 'tensor'), parts along dimension 0
- normed: bfloat16 [256, 8192], P(('groups', 'dp', 'seq')), parts along dimension 0
The draws below stay inside these ranges and needn't reach their ends.
There are 2 independent parts, one for each index of `groups`. The reference program is written for one: setup_inputs(seed, part) draws one part's arguments, and reference() takes and returns one part's arrays. A program takes and returns all parts, laid end to end along the dimension named above; an argument that names none is the same for every part. Nothing has to cross between parts.
All inputs are finite; a program needn't handle non-finite values.
Results may differ from the reference program's by a relative error of at most 0.0056.
Values may be sent and summed in bfloat16 or wider, within the bound.
A program may use at most 64 MiB of HBM per device.

```python
import math
import jax
import jax.numpy as jnp
from jax import lax

D = 8192
BATCH = 128


def draw_residual(key, part):
    key = jax.random.fold_in(key, 7)
    k_row, k_col, k_base = jax.random.split(key, 3)
    row_scale = jnp.exp(jax.random.uniform(k_row, (BATCH, 1), jnp.float32, math.log(0.2), math.log(2.0)))
    ramp = 1.0 + 0.8 * jnp.arange(D, dtype=jnp.float32) / D
    col_scale = ramp[None, :] * jnp.exp(jax.random.uniform(k_col, (1, D), jnp.float32, math.log(0.4), math.log(2.2)))
    base = jax.random.normal(k_base, (BATCH, D), jnp.float32)
    return jnp.clip(row_scale * col_scale * base, -32.0, 32.0).astype(jnp.bfloat16)


def with_spikes(values, rng, source, target, shards_of, factor):
    def block_of(dim):
        return (jnp.arange(values.shape[dim]) // (values.shape[dim] // shards_of)).reshape((-1,) + (1,) * (values.ndim - 1 - dim))

    near = jax.random.permutation(rng, shards_of)[block_of(target)]
    second = (block_of(target) + shards_of // 2) % shards_of
    return jnp.where((block_of(source) == near) | (block_of(source) == second), factor * values, values)


def shard_levels(rng, extent, cuts, low, largest):
    def one(axis_at, blocks):
        draws = jax.random.uniform(jax.random.fold_in(jax.random.fold_in(rng, 6), axis_at), (blocks,), jnp.float32, low / len(cuts), largest / len(cuts))
        return jnp.repeat(jnp.exp(draws), extent[axis_at] // blocks).reshape((-1,) + (1,) * (len(extent) - axis_at - 1))

    level = one(*cuts[0])
    for cut in cuts[1:]:
        level = level * one(*cut)
    return level


def gaussian(key, dims, scale, reach, shards=(), held_as=jnp.bfloat16):
    entries = jax.random.normal(key, dims, jnp.float32) * scale
    if len(shards) > 0:
        entries = shard_levels(key, dims, shards, -0.22, 0.18) * entries
    return jnp.clip(entries, min=-reach, max=reach).astype(held_as)


def heavy_noise(rng, dims, scale, bound, cuts, heavy, kind=jnp.bfloat16):
    result = scale * jax.random.normal(rng, dims, jnp.float32)
    if cuts:
        result = result * shard_levels(rng, dims, cuts, -0.22, 0.18)
    return jnp.clip(with_spikes(result, jax.random.fold_in(rng, 3), *heavy), -bound, bound).astype(kind)


def setup_inputs(seed: int = 0, part: int = 0) -> dict:
    keys = jax.random.split(jax.random.key(seed), 5)
    part_splits = jax.random.split(jax.random.fold_in(keys[4], part), 5)
    return {
        "attn_heads": gaussian(part_splits[0], (BATCH, D), 1.0, 6.0, ((0, 4), (1, 4))),
        "out_weight": heavy_noise(keys[1], (D, D), D ** -0.5, 0.09375, ((0, 8),), (0, 1, 8, 2.0)),
        "residual": draw_residual(jax.random.fold_in(jax.random.fold_in(keys[4], part), 71), part),
        "norm_gain": jnp.clip(1.0 + 0.18 * jax.random.normal(keys[3], (D,), jnp.float32), 0.099609375, 1.8984375).astype(jnp.bfloat16),
    }


def reference(attn_heads, out_weight, residual, norm_gain):
    attended = jnp.dot(attn_heads, out_weight, preferred_element_type=jnp.float32)
    stream = (residual.astype(jnp.float32) + attended).astype(jnp.bfloat16)
    stream_float = stream.astype(jnp.float32)
    mean_square = lax.optimization_barrier(jnp.mean(stream_float * stream_float, axis=1, keepdims=True))
    normed = stream_float * lax.rsqrt(mean_square + 1e-05) * norm_gain.astype(jnp.float32)[None, :]
    return (stream, normed.astype(jnp.bfloat16))
```

```python
import functools

import jax
import jax.numpy as jnp
from jax import lax
from jax.experimental import pallas as pl
from jax.experimental.pallas import tpu as pltpu
from jax.sharding import PartitionSpec as P

MESH = pl.DeviceIdType.MESH
EPS = 1e-05
LAG = 3


def kernel(
    tensor_size, chunk, x_hbm, w_hbm, res_hbm, gain_hbm, stream_ref, normed_ref,
    x_keep, x_give, w_buf, res_buf, gains, core_out, core_in, own_part, part_out, part_in,
    full, squares,
    x_sem, w_sem, xs_sem, xr_sem, gs_sem, gr_sem, cs_sem, cr_sem, ps_sem, pr_sem, fs_sem, fr_sem,
):
    size = tensor_size
    pairs = size // 2
    z = lax.axis_index("tensor")
    core = lax.axis_index("seq")
    rows, width = res_hbm.shape
    depth, total = w_hbm.shape
    splits = width // chunk
    pair, parity = z // 2, lax.rem(z, 2)

    def peer(k):
        return {"tensor": lax.rem(z + k, size)}

    other_core = {"seq": 1 - core}

    order = [(s, k) for s in range(splits) for k in list(range(1, size)) + [0]]

    def x_cols(which):
        return pl.ds(pl.multiple_of(which * depth, depth), depth)

    keep = pltpu.make_async_copy(x_hbm.at[:, x_cols(core)], x_keep.at[0], x_sem.at[0])
    give = pltpu.make_async_copy(x_hbm.at[:, x_cols(1 - core)], x_give, x_sem.at[1])
    give.start()
    keep.start()
    loads = []
    for i, (s, k) in enumerate(order):
        start = pl.multiple_of(lax.rem(z + k, size) * width + s * chunk, chunk)
        load = pltpu.make_async_copy(w_hbm.at[:, pl.ds(start, chunk)], w_buf.at[i], w_sem.at[i])
        load.start()
        loads.append(load)
        if i == 1:
            res_load = pltpu.make_async_copy(res_hbm, res_buf, x_sem.at[2])
            gain_load = pltpu.make_async_copy(gain_hbm, gains.at[z], x_sem.at[3])
            res_load.start()
            gain_load.start()

    barrier = pltpu.get_barrier_semaphore()
    pl.semaphore_signal(barrier, inc=1, device_id=other_core, device_id_type=MESH)
    for k in range(1, size):
        pl.semaphore_signal(barrier, inc=1, device_id=peer(k), device_id_type=MESH)
    give.wait()
    pl.semaphore_wait(barrier, size)

    swap = pltpu.make_async_remote_copy(
        x_give, x_keep.at[1], xs_sem, xr_sem, device_id=other_core, device_id_type=MESH
    )
    swap.start()
    sends = [swap]
    gain_load.wait()
    gain_copies = []
    for k in range(1, size):
        copy = pltpu.make_async_remote_copy(
            gains.at[z], gains.at[z], gs_sem.at[k], gr_sem.at[k], device_id=peer(k), device_id_type=MESH
        )
        copy.start()
        gain_copies.append(copy)
    keep.wait()
    swap.wait_recv()
    res_load.wait()

    x = x_keep[...].reshape(2 * rows, depth)
    core_copies = {}
    part_copies = {}
    count = len(order)
    for i in range(count + LAG):
        if i < count:
            loads[i].wait()
            product = jnp.dot(x, w_buf[i], preferred_element_type=jnp.float32)
            core_out[i] = product[rows:]
            own_part[i] = product[:rows]
            copy = pltpu.make_async_remote_copy(
                core_out.at[i], core_in.at[i], cs_sem.at[i], cr_sem.at[i],
                device_id=other_core, device_id_type=MESH,
            )
            copy.start()
            core_copies[i] = copy
        j = i - LAG
        if j >= 0:
            s, k = order[j]
            core_copies[j].wait_recv()
            both = own_part[j] + core_in[j]
            if k == 0:
                own_part[j] = both + res_buf[:, s * chunk:(s + 1) * chunk].astype(jnp.float32)
            else:
                part_out[k, s] = both.astype(jnp.bfloat16)
                copy = pltpu.make_async_remote_copy(
                    part_out.at[k, s], part_in.at[k, s], ps_sem.at[k, s], pr_sem.at[k, s],
                    device_id=peer(k), device_id_type=MESH,
                )
                copy.start()
                part_copies[k, s] = copy

    def note_squares(block, s, value):
        value = value.astype(jnp.float32)
        square = value * value
        squares[block, s] = functools.reduce(
            lambda a, b: a + b, [square[:, c:c + 128] for c in range(0, chunk, 128)]
        )

    gathers = []
    direct = {}
    for s in range(splits):
        at = order.index((s, 0))
        value = own_part[at]
        for k in range(1, size):
            part_copies[k, s].wait_recv()
            value = value + part_in[k, s].astype(jnp.float32)
        value = value.astype(jnp.bfloat16)
        full[z, s] = value
        for m in range(1, pairs):
            target = 2 * lax.rem(pair + m, pairs) + parity
            copy = pltpu.make_async_remote_copy(
                full.at[z, s], full.at[z, s],
                fs_sem.at[0, m, s], fr_sem.at[0, (pairs - m) % pairs, s],
                device_id={"tensor": target}, device_id_type=MESH,
            )
            copy.start()
            direct[(pairs - m) % pairs, s] = copy
        copy = pltpu.make_async_remote_copy(
            full.at[z, s], full.at[z, s], fs_sem.at[1, 0, s], fr_sem.at[1, 0, s],
            device_id={"tensor": 2 * pair + 1 - parity}, device_id_type=MESH,
        )
        copy.start()
        gathers.append((0, s, copy))
        stream_ref[:, s * chunk:(s + 1) * chunk] = value
        note_squares(z, s, value)

    for s in range(splits):
        for m in range(1, pairs):
            direct[m, s].wait_recv()
            block = 2 * lax.rem(pair + m, pairs) + parity
            copy = pltpu.make_async_remote_copy(
                full.at[block, s], full.at[block, s], fs_sem.at[1, m, s], fr_sem.at[1, m, s],
                device_id={"tensor": 2 * pair + 1 - parity}, device_id_type=MESH,
            )
            copy.start()
            gathers.append((m, s, copy))
            note_squares(block, s, full[block, s])
    for m, s, copy in gathers:
        copy.wait_recv()
        block = 2 * lax.rem(pair + m, pairs) + 1 - parity
        note_squares(block, s, full[block, s])

    summed = functools.reduce(
        lambda a, b: a + b, [squares[block, s] for block in range(size) for s in range(splits)]
    )
    scale = lax.rsqrt(jnp.sum(summed, axis=1, keepdims=True) / total + EPS)
    for copy in gain_copies:
        copy.wait_recv()
    for block in range(size):
        gain = gains[block].astype(jnp.float32)
        for s in range(splits):
            first = block * width + s * chunk
            normed_ref[:, first:first + chunk] = (
                full[block, s].astype(jnp.float32) * scale * gain[:, s * chunk:(s + 1) * chunk]
            ).astype(jnp.bfloat16)

    for copy in (
        sends + gain_copies + list(core_copies.values()) + list(part_copies.values())
        + list(direct.values()) + [copy for _, _, copy in gathers]
    ):
        copy.wait_send()


def on_device(attn_heads, out_weight, residual, norm_gain):
    rows, width = residual.shape
    depth, total = out_weight.shape
    size = total // width
    chunk = min(width, 512)
    splits = width // chunk
    count = size * splits
    half, single = jnp.bfloat16, jnp.float32
    any_space = pl.BlockSpec(memory_space=pl.ANY)
    vmem = pl.BlockSpec(memory_space=pltpu.VMEM)
    dma = pltpu.SemaphoreType.DMA
    return pl.pallas_call(
        functools.partial(kernel, size, chunk),
        out_shape=(
            jax.ShapeDtypeStruct((rows, width), half),
            jax.ShapeDtypeStruct((rows, total), half),
        ),
        in_specs=[any_space] * 4,
        out_specs=(vmem, vmem),
        scratch_shapes=[
            pltpu.VMEM((2, rows, depth), half),
            pltpu.VMEM((rows, depth), half),
            pltpu.VMEM((count, depth, chunk), half),
            pltpu.VMEM((rows, width), half),
            pltpu.VMEM((size, 1, width), half),
            pltpu.VMEM((count, rows, chunk), single),
            pltpu.VMEM((count, rows, chunk), single),
            pltpu.VMEM((count, rows, chunk), single),
            pltpu.VMEM((size, splits, rows, chunk), half),
            pltpu.VMEM((size, splits, rows, chunk), half),
            pltpu.VMEM((size, splits, rows, chunk), half),
            pltpu.VMEM((size, splits, rows, 128), single),
            dma((4,)),
            dma((count,)),
            dma,
            dma,
            dma((size,)),
            dma((size,)),
            dma((count,)),
            dma((count,)),
            dma((size, splits)),
            dma((size, splits)),
            dma((2, size // 2, splits)),
            dma((2, size // 2, splits)),
        ],
        compiler_params=pltpu.CompilerParams(
            collective_id=0, has_side_effects=True, vmem_limit_bytes=48 * 1024 * 1024
        ),
    )(attn_heads, out_weight, residual, norm_gain.reshape(1, width))


def solution(mesh):
    rows = P(("groups", "dp", "seq"), "tensor")
    in_specs = (rows, P(("tensor", "seq"), None), rows, P("tensor"))
    out_specs = (rows, P(("groups", "dp", "seq"), None))
    return jax.shard_map(
        on_device, mesh=mesh, in_specs=in_specs, out_specs=out_specs, check_vma=False
    )
```
